32 devices in a mesh: span: 32 (over z, y, x, core).
Axes of the slice: x: 2, y: 2, z: 4, core: 2. Of those that a mesh axis runs over, the one named last changes fastest.
Arguments:
- returns: bfloat16 [256, 262144], P(None, 'span'), may hold values from -40 to 40
- market: bfloat16 [262144], P('span'), may hold values from -12 to 12
- mask: int32 [262144], P('span'), may hold values 0 or 1
- counts: int32 [32], P('span'), may hold values from 0 to 8192, as said below
Outputs:
- slope: float32 [256, 131072], P(None, 'span')
The draws below stay inside these ranges and needn't reach their ends.
Inputs may be any that keep to these rules, and one draw needn't show every extreme that they name: For every span d, the counts of spans 0 to d sum to between (d + 1) * 4096 and (d + 2) * 4096; all counts sum to exactly 131072; some span holds exactly 8192.
All inputs are finite; a program needn't handle non-finite values. No bound on the sum of `mask` on one device may be relied on, other than what follows from the above.
Results may differ from the reference program's by a relative error of at most 0.00039.
Values may be sent and summed in bfloat16 or wider, within the bound.
A program may use at most 64 MiB of HBM per device.

```python
import jax
import jax.numpy as jnp
from jax import lax

STOCKS = 256
WIN = 1024
BLOCK = 512
QROWS = 4096
CAP = 8192
N_SPAN = 32


def series_parts(key):
    row_total = N_SPAN * 2 * QROWS
    subkeys = jax.random.split(jax.random.fold_in(key, 11), 4)
    market = jax.random.normal(subkeys[0], (row_total,), jnp.float32)
    noise_part = jax.random.normal(subkeys[1], (STOCKS, row_total), jnp.float32)
    market = jnp.clip(market, -12.0, 12.0)
    beta_load = jax.random.uniform(subkeys[2], (STOCKS, 1), jnp.float32, 0.4, 1.8)
    regime = 1.0 + 0.6 * jax.random.uniform(subkeys[3], (STOCKS, row_total // BLOCK), jnp.float32, -1.0, 1.0)
    regime = jnp.repeat(regime, BLOCK, axis=1)
    returns = jnp.clip(beta_load * regime * market[None, :] + noise_part, -40.0, 40.0)
    return (returns, market)


def draw_returns(key, part):
    return series_parts(key)[0].astype(jnp.bfloat16)


def draw_market(key, part):
    return series_parts(key)[1].astype(jnp.bfloat16)


def draw_counts(key, part):
    excess = jax.random.randint(jax.random.fold_in(key, 3), (N_SPAN,), 0, QROWS + 1)
    excess = excess.at[N_SPAN - 3].set(QROWS)
    chosen = jax.random.randint(jax.random.fold_in(key, 5), (), 1, N_SPAN - 2)
    excess = excess.at[chosen].set(QROWS)
    excess = excess.at[chosen - 1].set(0)
    excess = excess.at[N_SPAN - 1].set(0)
    previous = jnp.concatenate([jnp.zeros((1,), jnp.int32), excess[:-1]])
    return (QROWS + excess - previous).astype(jnp.int32)


def plant(result, stream_key, least, top_value):
    dims = result.shape
    index_at = [jax.random.randint(jax.random.fold_in(stream_key, axis), (), 0, dims[axis]) for axis in range(len(dims))]
    result = result.at[tuple(index_at)].set(least)
    longest = dims.index(max(dims))
    index_at[longest] = (index_at[longest] + 1) % dims[longest]
    return result.at[tuple(index_at)].set(top_value)


def setup_inputs(seed: int = 0) -> dict:
    seeds = jax.random.split(jax.random.key(seed), 5)
    return {
        "returns": draw_returns(jax.random.fold_in(seeds[4], 71), 0),
        "market": draw_market(jax.random.fold_in(seeds[4], 71), 0),
        "mask": plant((jax.random.randint(seeds[2], (N_SPAN * CAP,), 0, 8) < 7).astype(jnp.int32), jax.random.fold_in(seeds[2], 1), 0, 1),
        "counts": draw_counts(jax.random.fold_in(seeds[4], 71), 0),
    }


RIDGE = 0.1


def band_matrix():
    row_index = jnp.arange(BLOCK + WIN, dtype=jnp.int32)[:, None]
    col_index = jnp.arange(BLOCK, dtype=jnp.int32)[None, :]
    inside = (row_index >= col_index + 1) & (row_index <= col_index + WIN)
    return inside.astype(jnp.bfloat16)


def stacked(y_values, x_values, w_values):
    cross_terms = (x_values.astype(jnp.float32)[None, :] * y_values.astype(jnp.float32)).astype(jnp.bfloat16)
    square = (x_values.astype(jnp.float32) * x_values.astype(jnp.float32)).astype(jnp.bfloat16)
    return jnp.concatenate([cross_terms, y_values, w_values[None, :], x_values[None, :], square[None, :]], 0)


def slopes_of(moments):
    stocks = (moments.shape[0] - 3) // 2
    sum_xy = moments[:stocks]
    sum_y = moments[stocks:2 * stocks]
    sum_w = moments[2 * stocks]
    sum_x = moments[2 * stocks + 1]
    sum_xx = moments[2 * stocks + 2]
    numerator = sum_w * sum_xy - sum_x * sum_y
    denominator = sum_w * sum_xx - sum_x * sum_x + RIDGE * WIN * WIN
    return numerator / denominator


def reference(returns, market, mask, counts):
    capacity = 2 * QROWS
    tick_total = QROWS * N_SPAN
    before = (jnp.cumsum(counts) - counts).astype(jnp.int32)
    row_index = jnp.arange(capacity, dtype=jnp.int32)
    destination = before[:, None] + row_index[None, :]
    destination = jnp.where(row_index[None, :] < counts[:, None], destination, tick_total).reshape(-1).astype(jnp.int32)
    weight = mask.astype(jnp.float32)
    y_values = (returns.astype(jnp.float32) * weight[None, :]).astype(jnp.bfloat16)
    x_values = (market.astype(jnp.float32) * weight).astype(jnp.bfloat16)
    y_ticks = jnp.zeros((STOCKS, tick_total), jnp.bfloat16).at[:, destination].set(y_values, mode="drop")
    x_ticks = jnp.zeros((tick_total,), jnp.bfloat16).at[destination].set(x_values, mode="drop")
    w_ticks = jnp.zeros((tick_total,), jnp.bfloat16).at[destination].set(weight.astype(jnp.bfloat16), mode="drop")
    stacked_rows = stacked(y_ticks, x_ticks, w_ticks)
    extended = jnp.concatenate([jnp.zeros((stacked_rows.shape[0], WIN), jnp.bfloat16), stacked_rows], 1)
    band_ones = band_matrix()

    def one_block(block_index):
        window_piece = lax.dynamic_slice_in_dim(extended, block_index * BLOCK, BLOCK + WIN, 1)
        return slopes_of(jnp.dot(window_piece, band_ones, preferred_element_type=jnp.float32))

    blocks = lax.map(one_block, jnp.arange(tick_total // BLOCK, dtype=jnp.int32))
    return jnp.transpose(blocks, (1, 0, 2)).reshape(STOCKS, tick_total)
```

```python
import functools

import jax
import jax.numpy as jnp
from jax import lax
from jax.experimental import pallas as pl
from jax.experimental.pallas import tpu as pltpu
from jax.sharding import PartitionSpec as P

WIN = 1024
RIDGE = 0.1
LANE = 128
STEP = 256
EXTRA = 16
TAIL = WIN // LANE + 1
MESH = pl.DeviceIdType.MESH


def pack_kernel(body, tiles_ref, own_ref, xw_ref, out_ref, sems):
    stocks = own_ref.shape[0]
    tiles = tiles_ref[0]
    before_tail = jnp.maximum(tiles - TAIL, 0)

    def copies(i):
        j = jnp.where(i < body, before_tail, tiles - TAIL) - body + i
        source = pl.ds(pl.multiple_of(jnp.maximum(j, 0) * LANE, LANE), LANE)
        target = pl.ds(pl.multiple_of(i * LANE, LANE), LANE)
        return (
            pltpu.make_async_copy(own_ref.at[:, source], out_ref.at[pl.ds(0, stocks), target], sems.at[0, i]),
            pltpu.make_async_copy(xw_ref.at[:, source], out_ref.at[pl.ds(stocks, EXTRA), target], sems.at[1, i]),
        )

    def begin(i, _):
        for copy in copies(i):
            copy.start()
        return 0

    def end(i, _):
        for copy in copies(i):
            copy.wait()
        return 0

    lax.fori_loop(0, body + TAIL, begin, 0)
    lax.fori_loop(0, body + TAIL, end, 0)


def exchange_kernel(n, body, packed_ref, spare_ref, count_ref, got_ref, counts_ref,
                    prev_buf, mine_buf, body_buf, small_send, small_recv,
                    sems_send, sems_recv, local_sems):
    me = lax.axis_index("span")
    right = lax.rem(me + 1, n)
    barrier = pltpu.get_barrier_semaphore()

    def greet(k, _):
        pl.semaphore_signal(barrier, inc=1, device_id=(lax.rem(me + k, n),), device_id_type=MESH)
        return 0

    lax.fori_loop(1, n, greet, 0)
    cut = TAIL * LANE
    mine = pltpu.make_async_copy(packed_ref.at[:, pl.ds(0, cut)], mine_buf, local_sems.at[0])
    mine.start()
    counts_ref[me] = count_ref[...]
    pl.semaphore_wait(barrier, n - 1)

    def part(index, first, width):
        return pltpu.make_async_remote_copy(
            src_ref=packed_ref.at[:, pl.ds(first, width)], dst_ref=got_ref.at[:, pl.ds(first, width)],
            send_sem=sems_send.at[index], recv_sem=sems_recv.at[index],
            device_id=(right,), device_id_type=MESH)

    tail_copy = part(0, body * LANE, cut)
    tail_copy.start()
    late_copy = part(1, cut, body * LANE - cut)
    late_copy.start()

    def small(k):
        return pltpu.make_async_remote_copy(
            src_ref=count_ref, dst_ref=counts_ref.at[me],
            send_sem=small_send.at[k], recv_sem=small_recv.at[k],
            device_id=(lax.rem(me + k, n),), device_id_type=MESH)

    def send_small(k, _):
        small(k).start()
        return 0

    lax.fori_loop(1, n, send_small, 0)
    mine.wait()
    tail_copy.wait_recv()
    fetch = pltpu.make_async_copy(got_ref.at[:, pl.ds(body * LANE, cut)], prev_buf, local_sems.at[1])
    fetch.start()
    fetch.wait()

    for i in range(TAIL):
        here = slice(i * LANE, (i + 1) * LANE)
        e = (TAIL - 1 - i) * LANE
        spare = spare_ref[0:1, here]
        body_buf[:, here] = mine_buf[:, here] * (1 - spare) + prev_buf[:, e:e + LANE] * spare

    body_copy = pltpu.make_async_remote_copy(
        src_ref=body_buf, dst_ref=got_ref.at[:, pl.ds(0, cut)],
        send_sem=sems_send.at[2], recv_sem=sems_recv.at[2],
        device_id=(right,), device_id_type=MESH)
    body_copy.start()

    def wait_small(k, _):
        small(k).wait()
        return 0

    lax.fori_loop(1, n, wait_small, 0)
    tail_copy.wait_send()
    late_copy.wait()
    body_copy.wait()


def regress_kernel(quota, body, own_ref, xw_ref, got_ref, counts_ref, me_ref, out_ref,
                   align_y, align_xw, tri, sums, carry):
    t = pl.program_id(0)
    lag = WIN // STEP
    me = me_ref[0]
    stocks = own_ref.shape[0]
    f32 = jnp.float32
    held = counts_ref[...].astype(f32)
    device = lax.broadcasted_iota(jnp.int32, held.shape, 0)

    def pick(condition):
        return jnp.max(jnp.sum(jnp.where(condition, held, 0.0), 0, keepdims=True)).astype(jnp.int32)

    own_count = pick(device == me)
    count_1 = pick(device == me - 1)
    count_2 = pick(device == me - 2)
    start = pick(device < me) - me * quota + WIN
    start_1 = start - count_1
    start_2 = start_1 - count_2
    tiles_1 = (count_1 + LANE - 1) // LANE
    tiles_2 = (count_2 + LANE - 1) // LANE
    gone = jnp.maximum(tiles_1 - TAIL, 0)

    @pl.when(t == 0)
    def _():
        k = lax.broadcasted_iota(jnp.int32, tri.shape, 0)
        col = lax.broadcasted_iota(jnp.int32, tri.shape, 1)
        tri[...] = jnp.where(k <= col, 1.0, 0.0).astype(jnp.bfloat16)
        carry[...] = jnp.zeros_like(carry)

    align_y[...] = jnp.zeros_like(align_y)
    align_xw[...] = jnp.zeros_like(align_xw)
    first = t * STEP
    width = STEP + LANE

    def add_piece(offset, low, high, columns, load):
        low_here = jnp.maximum(low, first - offset)
        high_here = jnp.minimum(high, first - offset + STEP)

        @pl.when(low_here < high_here)
        def _():
            tile = jnp.clip((first - offset + columns) // LANE - columns // LANE, 0, (columns - width) // LANE)
            at = pl.multiple_of(tile * LANE, LANE)
            c = lax.broadcasted_iota(jnp.int32, (width, STEP), 0) + at
            p = lax.broadcasted_iota(jnp.int32, (width, STEP), 1) + (first - offset)
            chosen = (c == p) & (c >= low) & (c < high)
            hot = jnp.where(chosen, 1.0, 0.0).astype(jnp.bfloat16)
            y, xw = load(pl.ds(at, width))
            align_y[...] += jnp.dot(y, hot, preferred_element_type=f32)
            align_xw[...] += jnp.dot(xw, hot, preferred_element_type=f32)

    def load_own(s):
        return own_ref[:, s], xw_ref[:, s]

    def load_got(s):
        return got_ref[pl.ds(0, stocks), s], got_ref[pl.ds(stocks, EXTRA), s]

    capacity = own_ref.shape[1]
    add_piece(start, 0, own_count, capacity, load_own)
    base = (body + TAIL - tiles_1) * LANE
    add_piece(start_1 - base, jnp.maximum(base, 0), base + count_1, got_ref.shape[1], load_got)
    free = jnp.minimum(body - gone, TAIL) * LANE

    @pl.when((t < lag) & (start_1 > first))
    def _():
        c = lax.broadcasted_iota(jnp.int32, (TAIL * LANE, STEP), 0)
        p = lax.broadcasted_iota(jnp.int32, (TAIL * LANE, STEP), 1) + (first - start_2)
        slot = c // LANE
        source = (tiles_2 - 1 - 2 * slot) * LANE + c
        chosen = (source == p) & (c < free) & (source >= 0) & (source < count_2)
        hot = jnp.where(chosen, 1.0, 0.0).astype(jnp.bfloat16)
        y, xw = load_got(pl.ds(0, TAIL * LANE))
        align_y[...] += jnp.dot(y, hot, preferred_element_type=f32)
        align_xw[...] += jnp.dot(xw, hot, preferred_element_type=f32)

    w = align_xw[1:2, :]
    x = align_xw[0:1, :] * w
    y = align_y[...] * w
    cross = (x * y).astype(jnp.bfloat16)
    square = (x * x).astype(jnp.bfloat16)
    row = lax.broadcasted_iota(jnp.int32, (EXTRA, STEP), 0)
    small = jnp.where(row == 0, w, jnp.where(row == 1, x, jnp.where(row == 2, square.astype(f32), 0.0)))
    slot = lax.rem(t, lag + 1)
    old = lax.rem(t + 1, lag + 1)

    def window(lo, size, value):
        rows = pl.ds(lo, size)
        now = jnp.dot(value.astype(jnp.bfloat16), tri[...], preferred_element_type=f32)
        before = jnp.where(t >= lag, sums[old, rows, :], 0.0)
        result = carry[rows, :] + (now - before)
        sums[slot, rows, :] = now
        carry[rows, :] = jnp.broadcast_to(result[:, STEP - 1:], (size, STEP))
        return result

    sum_small = window(2 * stocks, EXTRA, small)
    sum_w = sum_small[0:1]
    sum_x = sum_small[1:2]
    sum_xx = sum_small[2:3]
    sum_xy = window(0, stocks, cross)
    sum_y = window(stocks, stocks, y)
    numerator = sum_w * sum_xy - sum_x * sum_y
    denominator = sum_w * sum_xx - sum_x * sum_x + RIDGE * WIN * WIN
    out_ref[...] = numerator / denominator


def per_device(n, returns, market, mask, counts):
    stocks, capacity = returns.shape
    quota = capacity // 2
    body = quota // LANE + 1
    bf16 = jnp.bfloat16
    columns = (body + TAIL) * LANE
    rows = stocks + EXTRA
    xw = jnp.concatenate([market[None, :], mask.astype(bf16)[None, :],
                          jnp.zeros((EXTRA - 2, capacity), bf16)], 0)
    count_tile = jnp.broadcast_to(counts[:, None], (8, LANE))
    tiles = (counts + (LANE - 1)) // LANE
    slots = jnp.arange(TAIL * LANE, dtype=jnp.int32) // LANE
    free = (jnp.maximum(tiles - TAIL, 0) - body + slots < 0).astype(bf16)
    vmem = pl.BlockSpec(memory_space=pltpu.VMEM)
    hbm = pl.BlockSpec(memory_space=pltpu.HBM)
    packed = pl.pallas_call(
        functools.partial(pack_kernel, body),
        out_shape=jax.ShapeDtypeStruct((rows, columns), bf16),
        in_specs=[pl.BlockSpec(memory_space=pltpu.SMEM), hbm, hbm],
        out_specs=vmem,
        scratch_shapes=[pltpu.SemaphoreType.DMA((2, body + TAIL))],
        compiler_params=pltpu.CompilerParams(vmem_limit_bytes=16 * 2**20),
        name="pack",
    )(tiles, returns, xw)
    tail_shape = (rows, TAIL * LANE)
    got, gathered = pl.pallas_call(
        functools.partial(exchange_kernel, n, body),
        out_shape=(jax.ShapeDtypeStruct((rows, columns), bf16),
                   jax.ShapeDtypeStruct((n, 8, LANE), jnp.int32)),
        in_specs=[hbm, vmem, vmem],
        out_specs=(hbm, vmem),
        scratch_shapes=[
            pltpu.VMEM(tail_shape, bf16),
            pltpu.VMEM(tail_shape, bf16),
            pltpu.VMEM(tail_shape, bf16),
            pltpu.SemaphoreType.DMA((n,)),
            pltpu.SemaphoreType.DMA((n,)),
            pltpu.SemaphoreType.DMA((3,)),
            pltpu.SemaphoreType.DMA((3,)),
            pltpu.SemaphoreType.DMA((2,)),
        ],
        compiler_params=pltpu.CompilerParams(
            collective_id=0, has_side_effects=True, vmem_limit_bytes=16 * 2**20),
        name="exchange",
    )(packed, jnp.broadcast_to(free[None, :], (EXTRA, TAIL * LANE)), count_tile)
    me = lax.axis_index("span").astype(jnp.int32).reshape(1)
    steps = (quota + WIN) // STEP
    lag = WIN // STEP

    def whole(*shape):
        return pl.BlockSpec(shape, lambda t, me: (0,) * len(shape))

    return pl.pallas_call(
        lambda m, a, b, c, d, *rest: regress_kernel(quota, body, a, b, c, d, m, *rest),
        out_shape=jax.ShapeDtypeStruct((stocks, quota), jnp.float32),
        grid_spec=pltpu.PrefetchScalarGridSpec(
            num_scalar_prefetch=1,
            grid=(steps,),
            in_specs=[whole(stocks, capacity), whole(EXTRA, capacity), whole(rows, columns), whole(n, LANE)],
            out_specs=pl.BlockSpec((stocks, STEP), lambda t, me: (0, jnp.maximum(t - lag, 0))),
            scratch_shapes=[
                pltpu.VMEM((stocks, STEP), jnp.float32),
                pltpu.VMEM((EXTRA, STEP), jnp.float32),
                pltpu.VMEM((STEP, STEP), bf16),
                pltpu.VMEM((lag + 1, 2 * stocks + EXTRA, STEP), jnp.float32),
                pltpu.VMEM((2 * stocks + EXTRA, STEP), jnp.float32),
            ],
        ),
        compiler_params=pltpu.CompilerParams(vmem_limit_bytes=56 * 2**20),
        name="regress",
    )(me, returns, xw, got, gathered[:, 0, :])


def solution(mesh):
    return jax.shard_map(
        functools.partial(per_device, mesh.shape["span"]),
        mesh=mesh,
        in_specs=(P(None, "span"), P("span"), P("span"), P("span")),
        out_specs=P(None, "span"),
        check_vma=False,
    )
```

```python
import functools

import jax
import jax.numpy as jnp
from jax import lax
from jax.experimental import pallas as pl
from jax.experimental.pallas import tpu as pltpu
from jax.sharding import PartitionSpec as P

WIN = 1024
RIDGE = 0.1
LANE = 128
STEP = 256
SUBS = 2
HALF = 8
TAIL = WIN // LANE + 1
MESH = pl.DeviceIdType.MESH


def pack_kernel(body, count_ref, own_ref, market_ref, mask_ref,
                packed_ref, own_xw_ref, packed_xw_ref, spare_ref, tile_ref):
    count = count_ref[0]
    tiles = (count + (LANE - 1)) // LANE
    before_tail = jnp.maximum(tiles - TAIL, 0)
    dense = market_ref.shape[0]
    half = packed_xw_ref.shape[0] // 2
    own_xw_ref[pl.ds(0, dense), :] = market_ref[...].astype(jnp.float32)
    own_xw_ref[pl.ds(dense, dense), :] = mask_ref[...].astype(jnp.float32)
    packed_xw_ref[...] = jnp.zeros_like(packed_xw_ref)
    tile_ref[...] = jnp.full(tile_ref.shape, count, jnp.int32)

    def fill(i, _):
        j = jnp.where(i < body, before_tail, tiles - TAIL) - body + i
        row = jnp.maximum(j, 0)
        source = pl.ds(pl.multiple_of(row * LANE, LANE), LANE)
        packed_ref[:, pl.ds(pl.multiple_of(i * LANE, LANE), LANE)] = own_ref[:, source]
        packed_xw_ref[pl.ds(i, 1), :] = own_xw_ref[pl.ds(row, 1), :]
        packed_xw_ref[pl.ds(half + i, 1), :] = own_xw_ref[pl.ds(dense + row, 1), :]
        return 0

    lax.fori_loop(0, body + TAIL, fill, 0)
    for i in range(TAIL):
        free = jnp.where(before_tail - body + i < 0, 1.0, 0.0)
        spare_ref[:, i * LANE:(i + 1) * LANE] = jnp.full((spare_ref.shape[0], LANE), free, jnp.float32)


def exchange_kernel(n, body, packed_ref, packed_xw_ref, spare_ref, count_ref,
                    got_ref, got_xw_ref, got_free_ref, counts_ref,
                    body_buf, free_buf, small_send, small_recv, sems_send, sems_recv):
    me = lax.axis_index("span")
    right = lax.rem(me + 1, n)
    barrier = pltpu.get_barrier_semaphore()

    def greet(k, _):
        pl.semaphore_signal(barrier, inc=1, device_id=(lax.rem(me + k, n),), device_id_type=MESH)
        return 0

    lax.fori_loop(1, n, greet, 0)
    cut = TAIL * LANE
    half = packed_xw_ref.shape[0] // 2
    half_free = free_buf.shape[0] // 2
    counts_ref[me] = count_ref[...]
    free_buf[...] = jnp.zeros_like(free_buf)
    pl.semaphore_wait(barrier, n - 1)

    def to_right(index, source, target):
        return pltpu.make_async_remote_copy(
            src_ref=source, dst_ref=target, send_sem=sems_send.at[index], recv_sem=sems_recv.at[index],
            device_id=(right,), device_id_type=MESH)

    def part(index, first, width):
        return to_right(index, packed_ref.at[:, pl.ds(first, width)], got_ref.at[:, pl.ds(first, width)])

    xw_copy = to_right(3, packed_xw_ref, got_xw_ref)
    xw_copy.start()
    tail_copy = part(0, body * LANE, cut)
    tail_copy.start()
    late_copy = part(1, cut, body * LANE - cut)
    late_copy.start()

    def small(k):
        return pltpu.make_async_remote_copy(
            src_ref=count_ref, dst_ref=counts_ref.at[me],
            send_sem=small_send.at[k], recv_sem=small_recv.at[k],
            device_id=(lax.rem(me + k, n),), device_id_type=MESH)

    def send_small(k, _):
        small(k).start()
        return 0

    lax.fori_loop(1, n, send_small, 0)
    xw_copy.wait_recv()
    tail_copy.wait_recv()

    for i in range(TAIL):
        here = slice(i * LANE, (i + 1) * LANE)
        row = body + TAIL - 1 - i
        free = spare_ref[0:1, here]
        spare = free.astype(jnp.bfloat16)
        body_buf[:, here] = packed_ref[:, here] * (1 - spare) + got_ref[:, row * LANE:(row + 1) * LANE] * spare
        free_buf[i:i + 1, :] = got_xw_ref[row:row + 1, :]
        free_buf[half_free + i:half_free + i + 1, :] = got_xw_ref[half + row:half + row + 1, :]

    body_copy = to_right(2, body_buf, got_ref.at[:, pl.ds(0, cut)])
    body_copy.start()
    free_copy = to_right(4, free_buf, got_free_ref)
    free_copy.start()

    def wait_small(k, _):
        small(k).wait()
        return 0

    lax.fori_loop(1, n, wait_small, 0)
    xw_copy.wait_send()
    tail_copy.wait_send()
    late_copy.wait()
    body_copy.wait()
    free_copy.wait()


def regress_kernel(quota, body, own_ref, own_xw_ref, got_ref, got_xw_ref, free_ref, counts_ref, out_ref,
                   facts, hot_own, hot_got, pair, align, history, small_history, carry):
    t = pl.program_id(0)
    me = lax.axis_index("span")
    stocks, capacity = own_ref.shape
    columns = got_ref.shape[1]
    f32, bf16 = jnp.float32, jnp.bfloat16
    width = STEP + LANE

    def hot_of(low, high, shift, rows):
        c = lax.broadcasted_iota(jnp.int32, (rows, STEP), 0)
        p = lax.broadcasted_iota(jnp.int32, (rows, STEP), 1)
        return jnp.where((c == p + shift) & (c >= low) & (c < high), 1.0, 0.0).astype(bf16)

    @pl.when(t == 0)
    def _():
        held = counts_ref[:, 0, :].astype(f32)
        device = lax.broadcasted_iota(jnp.int32, held.shape, 0)

        def pick(condition):
            return jnp.max(jnp.sum(jnp.where(condition, held, 0.0), 0, keepdims=True)).astype(jnp.int32)

        own_count = pick(device == me)
        count_1 = pick(device == me - 1)
        count_2 = pick(device == me - 2)
        start = pick(device < me) - me * quota + WIN
        facts[0] = own_count
        facts[1] = count_1
        facts[2] = count_2
        facts[3] = start
        base = (body + TAIL - (count_1 + LANE - 1) // LANE) * LANE
        hot_own[...] = hot_of(0, width, lax.rem(columns + LANE * LANE - start, LANE), width)
        hot_got[...] = hot_of(0, width, lax.rem(columns + LANE * LANE - (start - count_1 - base), LANE), width)
        k = lax.broadcasted_iota(jnp.int32, (STEP, STEP), 0)
        col = lax.broadcasted_iota(jnp.int32, (STEP, STEP), 1)
        pair[pl.ds(0, STEP), :] = jnp.where(k <= col, 1.0, 0.0).astype(bf16)
        pair[pl.ds(STEP, STEP), :] = jnp.where(k <= col, -1.0, 0.0).astype(bf16)
        carry[...] = jnp.zeros_like(carry)
        history[:, pl.ds(0, WIN)] = jnp.zeros((2 * stocks, WIN), bf16)
        small_history[:, pl.ds(0, WIN)] = jnp.zeros((HALF, WIN), f32)

    own_count = facts[0]
    count_1 = facts[1]
    count_2 = facts[2]
    start = facts[3]
    start_1 = start - count_1
    start_2 = start_1 - count_2
    tiles_1 = (count_1 + LANE - 1) // LANE
    tiles_2 = (count_2 + LANE - 1) // LANE
    base = (body + TAIL - tiles_1) * LANE
    free = jnp.minimum(body - jnp.maximum(tiles_1 - TAIL, 0), TAIL) * LANE
    dense = own_xw_ref.shape[0] // 2
    half = got_xw_ref.shape[0] // 2
    half_free = free_ref.shape[0] // 2

    def wide(ref, first_row, count):
        return jnp.concatenate([ref[pl.ds(first_row + i, 1), :] for i in range(count)], 1)

    def lift(y, x, w):
        row = lax.broadcasted_iota(jnp.int32, (16, x.shape[1]), 0)
        return jnp.concatenate([y, jnp.where(row == 0, x, w).astype(bf16)], 0)

    def load_own(tile):
        y = own_ref[:, pl.ds(pl.multiple_of(tile * LANE, LANE), width)]
        return lift(y, wide(own_xw_ref, tile, width // LANE), wide(own_xw_ref, dense + tile, width // LANE))

    def load_got(tile):
        y = got_ref[:, pl.ds(pl.multiple_of(tile * LANE, LANE), width)]
        return lift(y, wide(got_xw_ref, tile, width // LANE), wide(got_xw_ref, half + tile, width // LANE))

    def dot(a, b):
        return jnp.dot(a, b, preferred_element_type=f32)

    def gather(s):
        first = t * (SUBS * STEP) + s * STEP

        def plan(offset, low, high, total):
            head = first - offset
            floor = (head + columns) // LANE - columns // LANE
            tile = jnp.clip(floor, 0, (total - width) // LANE)
            inside = (low <= head) & (head + STEP <= high) & (tile == floor)
            touched = jnp.maximum(low, head) < jnp.minimum(high, head + STEP)
            at = tile * LANE
            return inside, touched, tile, (low - at, high - at, head - at)

        own_in, own_any, own_tile, own_map = plan(start, 0, own_count, capacity)
        got_in, got_any, got_tile, got_map = plan(
            start_1 - base, jnp.maximum(base, 0), base + count_1, columns)

        @pl.when(own_in)
        def _():
            align[s] = dot(load_own(own_tile), hot_own[...])

        @pl.when(got_in)
        def _():
            align[s] = dot(load_got(got_tile), hot_got[...])

        @pl.when(jnp.logical_not(own_in | got_in))
        def _():
            align[s] = jnp.zeros(align.shape[1:], f32)

            @pl.when(own_any)
            def _():
                align[s] += dot(load_own(own_tile), hot_of(*own_map, width))

            @pl.when(got_any)
            def _():
                align[s] += dot(load_got(got_tile), hot_of(*got_map, width))

            @pl.when((first < WIN) & (start_1 > first))
            def _():
                c = lax.broadcasted_iota(jnp.int32, (TAIL * LANE, STEP), 0)
                p = lax.broadcasted_iota(jnp.int32, (TAIL * LANE, STEP), 1) + (first - start_2)
                source = (tiles_2 - 1 - 2 * (c // LANE)) * LANE + c
                chosen = (source == p) & (c < free) & (source >= 0) & (source < count_2)
                hot = jnp.where(chosen, 1.0, 0.0).astype(bf16)
                align[s] += dot(lift(got_ref[:, pl.ds(0, TAIL * LANE)], wide(free_ref, 0, TAIL),
                                     wide(free_ref, half_free, TAIL)), hot)

    for s in range(SUBS):
        gather(s)

    small_rows = lax.broadcasted_iota(jnp.int32, (HALF, STEP), 0)
    moments = []
    both = pair[...]
    for s in range(SUBS):
        q = pl.multiple_of(t * (SUBS * STEP) + s * STEP, STEP)
        now_at = pl.ds(q + WIN, STEP)
        old_at = pl.ds(q, STEP)
        w = align[s, stocks + 1:stocks + 2, :]
        x = align[s, stocks:stocks + 1, :] * w
        y = align[s, 0:stocks, :] * w
        cross = (x * y).astype(bf16)
        y = y.astype(bf16)
        square = (x * x).astype(bf16).astype(f32)
        small = jnp.where(small_rows == 0, w, jnp.where(small_rows == 1, x, square))
        parts = []
        history[pl.ds(0, stocks), now_at] = cross
        history[pl.ds(stocks, stocks), now_at] = y
        small_history[:, now_at] = small
        pieces = (
            (0, stocks, cross, history[pl.ds(0, stocks), old_at]),
            (stocks, stocks, y, history[pl.ds(stocks, stocks), old_at]),
            (2 * stocks, HALF, small.astype(bf16), small_history[:, old_at].astype(bf16)),
        )
        for lo, size, now, old in pieces:
            change = dot(jnp.concatenate([now, old], 1), both)
            rows = pl.ds(lo, size)
            held = carry[rows, :]
            result = change + jnp.concatenate([held] * (STEP // LANE), 1)
            carry[rows, :] = jnp.broadcast_to(result[:, STEP - 1:], (size, LANE))
            parts.append(result)
        sum_xy, sum_y, tiny = parts
        sum_w = tiny[0:1]
        sum_x = tiny[1:2]
        sum_xx = tiny[2:3]
        inverse = 1.0 / (sum_w * sum_xx - sum_x * sum_x + RIDGE * WIN * WIN)
        out_ref[:, s * STEP:(s + 1) * STEP] = (sum_w * inverse) * sum_xy - (sum_x * inverse) * sum_y


def per_device(n, returns, market, mask, counts):
    stocks, capacity = returns.shape
    quota = capacity // 2
    body = quota // LANE + 1
    bf16, f32, i32 = jnp.bfloat16, jnp.float32, jnp.int32
    slots = body + TAIL
    columns = slots * LANE
    dense = capacity // LANE
    half = -(-slots // 8) * 8
    half_free = -(-TAIL // 8) * 8
    shape = jax.ShapeDtypeStruct
    vmem = pl.BlockSpec(memory_space=pltpu.VMEM)
    packed, own_xw, packed_xw, spare, count_tile = pl.pallas_call(
        functools.partial(pack_kernel, body),
        out_shape=(shape((stocks, columns), bf16), shape((2 * dense, LANE), f32), shape((2 * half, LANE), f32),
                   shape((8, TAIL * LANE), f32), shape((8, LANE), i32)),
        in_specs=[pl.BlockSpec(memory_space=pltpu.SMEM), vmem, vmem, vmem],
        out_specs=(vmem,) * 5,
        compiler_params=pltpu.CompilerParams(vmem_limit_bytes=16 * 2**20),
        name="pack",
    )(counts, returns, market.reshape(dense, LANE), mask.reshape(dense, LANE))
    got, got_xw, got_free, gathered = pl.pallas_call(
        functools.partial(exchange_kernel, n, body),
        out_shape=(shape((stocks, columns), bf16), shape((2 * half, LANE), f32),
                   shape((2 * half_free, LANE), f32), shape((n, 8, LANE), i32)),
        in_specs=[vmem] * 4,
        out_specs=(vmem,) * 4,
        scratch_shapes=[
            pltpu.VMEM((stocks, TAIL * LANE), bf16),
            pltpu.VMEM((2 * half_free, LANE), f32),
            pltpu.SemaphoreType.DMA((n,)),
            pltpu.SemaphoreType.DMA((n,)),
            pltpu.SemaphoreType.DMA((5,)),
            pltpu.SemaphoreType.DMA((5,)),
        ],
        compiler_params=pltpu.CompilerParams(
            collective_id=0, has_side_effects=True, vmem_limit_bytes=16 * 2**20),
        name="exchange",
    )(packed, packed_xw, spare, count_tile)
    steps = (quota + WIN) // (SUBS * STEP)
    lag = WIN // (SUBS * STEP)
    return pl.pallas_call(
        functools.partial(regress_kernel, quota, body),
        out_shape=shape((stocks, quota), f32),
        grid=(steps,),
        in_specs=[vmem] * 6,
        out_specs=pl.BlockSpec((stocks, SUBS * STEP), lambda t: (0, jnp.maximum(t - lag, 0))),
        scratch_shapes=[
            pltpu.SMEM((4,), i32),
            pltpu.VMEM((STEP + LANE, STEP), bf16),
            pltpu.VMEM((STEP + LANE, STEP), bf16),
            pltpu.VMEM((2 * STEP, STEP), bf16),
            pltpu.VMEM((SUBS, stocks + 16, STEP), f32),
            pltpu.VMEM((2 * stocks, quota + 2 * WIN), bf16),
            pltpu.VMEM((HALF, quota + 2 * WIN), f32),
            pltpu.VMEM((2 * stocks + HALF, LANE), f32),
        ],
        compiler_params=pltpu.CompilerParams(vmem_limit_bytes=32 * 2**20),
        name="regress",
    )(returns, own_xw, got, got_xw, got_free, gathered)


def solution(mesh):
    return jax.shard_map(
        functools.partial(per_device, mesh.shape["span"]),
        mesh=mesh,
        in_specs=(P(None, "span"), P("span"), P("span"), P("span")),
        out_specs=P(None, "span"),
        check_vma=False,
    )
```

```python
import functools

import jax
import jax.numpy as jnp
from jax import lax
from jax.experimental import pallas as pl
from jax.experimental.pallas import tpu as pltpu
from jax.sharding import PartitionSpec as P

WIN = 1024
RIDGE = 0.1
LANE = 128
STEP = 256
SUBS = WIN // STEP
HALF = 16
TAIL = WIN // LANE + 1
MESH = pl.DeviceIdType.MESH


def pack_kernel(body, count_ref, own_ref, own_x_ref, own_w_ref,
                packed_ref, packed_xw_ref, spare_ref, tile_ref):
    count = count_ref[0]
    tiles = (count + (LANE - 1)) // LANE
    before_tail = jnp.maximum(tiles - TAIL, 0)
    half = packed_xw_ref.shape[0] // 2
    packed_xw_ref[...] = jnp.zeros_like(packed_xw_ref)
    tile_ref[...] = jnp.full(tile_ref.shape, count, jnp.int32)

    def fill(i, _):
        j = jnp.where(i < body, before_tail, tiles - TAIL) - body + i
        row = jnp.maximum(j, 0)
        source = pl.ds(pl.multiple_of(row * LANE, LANE), LANE)
        packed_ref[:, pl.ds(pl.multiple_of(i * LANE, LANE), LANE)] = own_ref[:, source]
        packed_xw_ref[pl.ds(i, 1), :] = own_x_ref[pl.ds(row, 1), :]
        packed_xw_ref[pl.ds(half + i, 1), :] = own_w_ref[pl.ds(row, 1), :]
        return 0

    lax.fori_loop(0, body + TAIL, fill, 0)
    for i in range(TAIL):
        free = jnp.where(before_tail - body + i < 0, 1.0, 0.0)
        spare_ref[:, i * LANE:(i + 1) * LANE] = jnp.full((spare_ref.shape[0], LANE), free, jnp.float32)


def exchange_kernel(n, body, packed_ref, packed_xw_ref, spare_ref, count_ref,
                    got_ref, got_xw_ref, got_free_ref, counts_ref,
                    body_buf, free_buf, small_send, small_recv, sems_send, sems_recv):
    me = lax.axis_index("span")
    right = lax.rem(me + 1, n)
    barrier = pltpu.get_barrier_semaphore()

    def greet(k, _):
        pl.semaphore_signal(barrier, inc=1, device_id=(lax.rem(me + k, n),), device_id_type=MESH)
        return 0

    lax.fori_loop(1, n, greet, 0)
    cut = TAIL * LANE
    half = packed_xw_ref.shape[0] // 2
    half_free = free_buf.shape[0] // 2
    counts_ref[me] = count_ref[...]
    free_buf[...] = jnp.zeros_like(free_buf)
    pl.semaphore_wait(barrier, n - 1)

    def to_right(index, source, target):
        return pltpu.make_async_remote_copy(
            src_ref=source, dst_ref=target, send_sem=sems_send.at[index], recv_sem=sems_recv.at[index],
            device_id=(right,), device_id_type=MESH)

    def part(index, first, width):
        return to_right(index, packed_ref.at[:, pl.ds(first, width)], got_ref.at[:, pl.ds(first, width)])

    xw_copy = to_right(3, packed_xw_ref, got_xw_ref)
    xw_copy.start()
    tail_copy = part(0, body * LANE, cut)
    tail_copy.start()
    late_copy = part(1, cut, body * LANE - cut)
    late_copy.start()

    def small(k):
        return pltpu.make_async_remote_copy(
            src_ref=count_ref, dst_ref=counts_ref.at[me],
            send_sem=small_send.at[k], recv_sem=small_recv.at[k],
            device_id=(lax.rem(me + k, n),), device_id_type=MESH)

    def send_small(k, _):
        small(k).start()
        return 0

    lax.fori_loop(1, n, send_small, 0)
    xw_copy.wait_recv()
    tail_copy.wait_recv()

    for i in range(TAIL):
        here = slice(i * LANE, (i + 1) * LANE)
        row = body + TAIL - 1 - i
        free = spare_ref[0:1, here]
        spare = free.astype(jnp.bfloat16)
        body_buf[:, here] = packed_ref[:, here] * (1 - spare) + got_ref[:, row * LANE:(row + 1) * LANE] * spare
        free_buf[i:i + 1, :] = got_xw_ref[row:row + 1, :]
        free_buf[half_free + i:half_free + i + 1, :] = got_xw_ref[half + row:half + row + 1, :]

    body_copy = to_right(2, body_buf, got_ref.at[:, pl.ds(0, cut)])
    body_copy.start()
    free_copy = to_right(4, free_buf, got_free_ref)
    free_copy.start()

    def wait_small(k, _):
        small(k).wait()
        return 0

    lax.fori_loop(1, n, wait_small, 0)
    xw_copy.wait_send()
    tail_copy.wait_send()
    late_copy.wait()
    body_copy.wait()
    free_copy.wait()


def regress_kernel(quota, body, own_ref, own_x_ref, own_w_ref, got_ref, got_xw_ref, free_ref, counts_ref, out_ref,
                   facts, hot_own, hot_got, pair, ones, align, history, carry):
    t = pl.program_id(0)
    me = lax.axis_index("span")
    stocks, capacity = own_ref.shape
    columns = got_ref.shape[1]
    f32, bf16 = jnp.float32, jnp.bfloat16
    width = STEP + LANE

    def hot_of(low, high, shift, rows):
        c = lax.broadcasted_iota(jnp.int32, (rows, STEP), 0)
        p = lax.broadcasted_iota(jnp.int32, (rows, STEP), 1)
        return jnp.where((c == p + shift) & (c >= low) & (c < high), 1.0, 0.0).astype(bf16)

    @pl.when(t == 0)
    def _():
        held = counts_ref[:, 0, :].astype(f32)
        device = lax.broadcasted_iota(jnp.int32, held.shape, 0)

        def pick(condition):
            return jnp.max(jnp.sum(jnp.where(condition, held, 0.0), 0, keepdims=True)).astype(jnp.int32)

        own_count = pick(device == me)
        count_1 = pick(device == me - 1)
        count_2 = pick(device == me - 2)
        start = pick(device < me) - me * quota + WIN
        facts[0] = own_count
        facts[1] = count_1
        facts[2] = count_2
        facts[3] = start
        base = (body + TAIL - (count_1 + LANE - 1) // LANE) * LANE
        hot_own[...] = hot_of(0, width, lax.rem(columns + LANE * LANE - start, LANE), width)
        hot_got[...] = hot_of(0, width, lax.rem(columns + LANE * LANE - (start - count_1 - base), LANE), width)
        k = lax.broadcasted_iota(jnp.int32, (STEP, STEP), 0)
        col = lax.broadcasted_iota(jnp.int32, (STEP, STEP), 1)
        pair[pl.ds(0, STEP), :] = jnp.where(k <= col, 1.0, 0.0).astype(bf16)
        pair[pl.ds(STEP, STEP), :] = jnp.where(k <= col, -1.0, 0.0).astype(bf16)
        ones[...] = jnp.ones_like(ones)

    own_count = facts[0]
    count_1 = facts[1]
    count_2 = facts[2]
    start = facts[3]
    start_1 = start - count_1
    start_2 = start_1 - count_2
    tiles_1 = (count_1 + LANE - 1) // LANE
    tiles_2 = (count_2 + LANE - 1) // LANE
    base = (body + TAIL - tiles_1) * LANE
    free = jnp.minimum(body - jnp.maximum(tiles_1 - TAIL, 0), TAIL) * LANE
    half = got_xw_ref.shape[0] // 2
    half_free = free_ref.shape[0] // 2

    def wide(ref, first_row, count):
        return jnp.concatenate([ref[pl.ds(first_row + i, 1), :] for i in range(count)], 1)

    def lift(y, x, w):
        row = lax.broadcasted_iota(jnp.int32, (16, x.shape[1]), 0)
        return jnp.concatenate([y, jnp.where(row == 0, x, w).astype(bf16)], 0)

    def load_own(tile):
        y = own_ref[:, pl.ds(pl.multiple_of(tile * LANE, LANE), width)]
        return lift(y, wide(own_x_ref, tile, width // LANE), wide(own_w_ref, tile, width // LANE))

    def load_got(tile):
        y = got_ref[:, pl.ds(pl.multiple_of(tile * LANE, LANE), width)]
        return lift(y, wide(got_xw_ref, tile, width // LANE), wide(got_xw_ref, half + tile, width // LANE))

    def dot(a, b):
        return jnp.dot(a, b, preferred_element_type=f32)

    def plan(first, length, offset, low, high, total):
        head = first - offset
        floor = (head + columns) // LANE - columns // LANE
        reach = length + LANE
        tile = jnp.clip(floor, 0, (total - reach) // LANE)
        inside = (low <= head) & (head + length <= high) & (tile == floor)
        touched = jnp.maximum(low, head) < jnp.minimum(high, head + length)
        at = tile * LANE
        return inside, touched, tile, (low - at, high - at, head - at)

    def plan_own(first, length):
        return plan(first, length, start, 0, own_count, capacity)

    def plan_got(first, length):
        return plan(first, length, start_1 - base, jnp.maximum(base, 0), base + count_1, columns)

    def gather_all(load, tile, hot):
        pieces = jnp.concatenate([load(tile + s * (STEP // LANE)) for s in range(SUBS)], 0)
        result = dot(pieces, hot)
        for s in range(SUBS):
            align[s] = result[s * (stocks + 16):(s + 1) * (stocks + 16)]

    def gather(s):
        first = t * WIN + s * STEP
        own_in, own_any, own_tile, own_map = plan_own(first, STEP)
        got_in, got_any, got_tile, got_map = plan_got(first, STEP)

        @pl.when(own_in)
        def _():
            align[s] = dot(load_own(own_tile), hot_own[...])

        @pl.when(got_in)
        def _():
            align[s] = dot(load_got(got_tile), hot_got[...])

        @pl.when(jnp.logical_not(own_in | got_in))
        def _():
            align[s] = jnp.zeros(align.shape[1:], f32)

            @pl.when(own_any)
            def _():
                align[s] += dot(load_own(own_tile), hot_of(*own_map, width))

            @pl.when(got_any)
            def _():
                align[s] += dot(load_got(got_tile), hot_of(*got_map, width))

            @pl.when((first < WIN) & (start_1 > first))
            def _():
                c = lax.broadcasted_iota(jnp.int32, (TAIL * LANE, STEP), 0)
                p = lax.broadcasted_iota(jnp.int32, (TAIL * LANE, STEP), 1) + (first - start_2)
                source = (tiles_2 - 1 - 2 * (c // LANE)) * LANE + c
                chosen = (source == p) & (c < free) & (source >= 0) & (source < count_2)
                hot = jnp.where(chosen, 1.0, 0.0).astype(bf16)
                align[s] += dot(lift(got_ref[:, pl.ds(0, TAIL * LANE)], wide(free_ref, 0, TAIL),
                                     wide(free_ref, half_free, TAIL)), hot)

    all_own, _, all_own_tile, _ = plan_own(t * WIN, WIN)
    all_got, _, all_got_tile, _ = plan_got(t * WIN, WIN)

    @pl.when(all_own)
    def _():
        gather_all(load_own, all_own_tile, hot_own[...])

    @pl.when(all_got)
    def _():
        gather_all(load_got, all_got_tile, hot_got[...])

    @pl.when(jnp.logical_not(all_own | all_got))
    def _():
        for s in range(SUBS):
            gather(s)

    now = lax.rem(t, 2)
    old = 1 - now
    small_rows = lax.broadcasted_iota(jnp.int32, (HALF, STEP), 0)
    for s in range(SUBS):
        at = slice(s * STEP, (s + 1) * STEP)
        w = align[s, stocks + 1:stocks + 2, :]
        x = align[s, stocks:stocks + 1, :] * w
        y = align[s, 0:stocks, :] * w
        square = (x * x).astype(bf16).astype(f32)
        small = jnp.where(small_rows == 0, w, jnp.where(small_rows == 1, x, square))
        history[now, 0:stocks, at] = (x * y).astype(bf16)
        history[now, stocks:2 * stocks, at] = y.astype(bf16)
        history[now, 2 * stocks:2 * stocks + HALF, at] = small.astype(bf16)

    @pl.when(t == 0)
    def _():
        carry[...] = dot(history[now], ones[...])

    @pl.when(t > 0)
    def _():
        total = 2 * stocks + HALF
        pieces = jnp.concatenate([
            jnp.concatenate([history[now, :, s * STEP:(s + 1) * STEP], history[old, :, s * STEP:(s + 1) * STEP]], 1)
            for s in range(SUBS)], 0)
        change = dot(pieces, pair[...])

        def summed(s, lo, size):
            rows = pl.ds(lo, size)
            result = change[s * total + lo:s * total + lo + size] + jnp.concatenate(
                [carry[rows, :]] * (STEP // LANE), 1)
            carry[rows, :] = jnp.broadcast_to(result[:, STEP - 1:], (size, LANE))
            return result

        for s in range(SUBS):
            tiny = summed(s, 2 * stocks, HALF)
            sum_w = tiny[0:1]
            sum_x = tiny[1:2]
            sum_xx = tiny[2:3]
            inverse = 1.0 / (sum_w * sum_xx - sum_x * sum_x + RIDGE * WIN * WIN)
            sum_xy = summed(s, 0, stocks)
            sum_y = summed(s, stocks, stocks)
            out_ref[:, s * STEP:(s + 1) * STEP] = (sum_w * inverse) * sum_xy - (sum_x * inverse) * sum_y


def per_device(n, returns, market, mask, counts):
    stocks, capacity = returns.shape
    quota = capacity // 2
    body = quota // LANE + 1
    bf16, f32, i32 = jnp.bfloat16, jnp.float32, jnp.int32
    slots = body + TAIL
    columns = slots * LANE
    dense = capacity // LANE
    half = -(-slots // 8) * 8
    half_free = -(-TAIL // 8) * 8
    shape = jax.ShapeDtypeStruct
    vmem = pl.BlockSpec(memory_space=pltpu.VMEM)
    own_x = market.reshape(dense, LANE).astype(f32)
    own_w = mask.reshape(dense, LANE).astype(f32)
    packed, packed_xw, spare, count_tile = pl.pallas_call(
        functools.partial(pack_kernel, body),
        out_shape=(shape((stocks, columns), bf16), shape((2 * half, LANE), f32),
                   shape((8, TAIL * LANE), f32), shape((8, LANE), i32)),
        in_specs=[pl.BlockSpec(memory_space=pltpu.SMEM), vmem, vmem, vmem],
        out_specs=(vmem,) * 4,
        compiler_params=pltpu.CompilerParams(vmem_limit_bytes=16 * 2**20),
        name="pack",
    )(counts, returns, own_x, own_w)
    got, got_xw, got_free, gathered = pl.pallas_call(
        functools.partial(exchange_kernel, n, body),
        out_shape=(shape((stocks, columns), bf16), shape((2 * half, LANE), f32),
                   shape((2 * half_free, LANE), f32), shape((n, 8, LANE), i32)),
        in_specs=[vmem] * 4,
        out_specs=(vmem,) * 4,
        scratch_shapes=[
            pltpu.VMEM((stocks, TAIL * LANE), bf16),
            pltpu.VMEM((2 * half_free, LANE), f32),
            pltpu.SemaphoreType.DMA((n,)),
            pltpu.SemaphoreType.DMA((n,)),
            pltpu.SemaphoreType.DMA((5,)),
            pltpu.SemaphoreType.DMA((5,)),
        ],
        compiler_params=pltpu.CompilerParams(
            collective_id=0, has_side_effects=True, vmem_limit_bytes=16 * 2**20),
        name="exchange",
    )(packed, packed_xw, spare, count_tile)
    steps = (quota + WIN) // (SUBS * STEP)
    lag = WIN // (SUBS * STEP)
    return pl.pallas_call(
        functools.partial(regress_kernel, quota, body),
        out_shape=shape((stocks, quota), f32),
        grid=(steps,),
        in_specs=[vmem] * 7,
        out_specs=pl.BlockSpec((stocks, SUBS * STEP), lambda t: (0, jnp.maximum(t - lag, 0))),
        scratch_shapes=[
            pltpu.SMEM((4,), i32),
            pltpu.VMEM((STEP + LANE, STEP), bf16),
            pltpu.VMEM((STEP + LANE, STEP), bf16),
            pltpu.VMEM((2 * STEP, STEP), bf16),
            pltpu.VMEM((WIN, LANE), bf16),
            pltpu.VMEM((SUBS, stocks + 16, STEP), f32),
            pltpu.VMEM((2, 2 * stocks + HALF, WIN), bf16),
            pltpu.VMEM((2 * stocks + HALF, LANE), f32),
        ],
        compiler_params=pltpu.CompilerParams(vmem_limit_bytes=32 * 2**20),
        name="regress",
    )(returns, own_x, own_w, got, got_xw, got_free, gathered)


def solution(mesh):
    return jax.shard_map(
        functools.partial(per_device, mesh.shape["span"]),
        mesh=mesh,
        in_specs=(P(None, "span"), P("span"), P("span"), P("span")),
        out_specs=P(None, "span"),
        check_vma=False,
    )
```
